32 devices in a mesh: section: 8 (over z, core), board: 4 (over y, x).
Axes of the slice: x: 2, y: 2, z: 4, core: 2. Of those that a mesh axis runs over, the one named last changes fastest.
Arguments:
- root_reach: float32 [2, 8, 1326], replicated, may hold values from 0.05 to 1
- frontier_value: float32 [2, 8, 1326], replicated, may hold values from -60 to 60
- regret_stop: float32 [8, 16, 8, 1326], P('section', 'board'), may hold values from 1 to 30
- regret_go: float32 [8, 16, 8, 1326], P('section', 'board'), may hold values from 1 to 30
- board_live: int32 [16], P('board'), may hold values from 0 to 1, as said below
- board_cards: int32 [16, 5], P('board'), may hold values from 0 to 51, as said below
- hand_rank: int32 [16, 1326], P('board'), may hold values from 0 to 1325
Outputs:
- new_stop: float32 [8, 16, 8, 1326], P('section', 'board')
- new_go: float32 [8, 16, 8, 1326], P('section', 'board')
- section_values: float32 [8, 2, 8, 1326], P('section')
The draws below stay inside these ranges and needn't reach their ends.
Inputs may be any that keep to these rules, and one draw needn't show every extreme that they name: `board_live`: 0 or 1; among each device's 4 slots the first one is always 1. `board_cards`: a slot's 5 cards are distinct. `hand_rank`: equal values tie.
All inputs are finite; a program needn't handle non-finite values.
Results may differ from the reference program's by a relative error of at most 0.0008.
Values sent between devices are 32-bit elements; how exact they have to be, the bound alone decides.
A program may use at most 64 MiB of HBM per device.

```python
import math
import jax
import jax.numpy as jnp
import numpy as np
from jax import lax

CARDS = 52
BOARD_CARDS = 5
H = 1326
NODES = 8
BOARD_DEV = 4
SLOTS = 16
SECTIONS = 8


def draw_board_cards(key, part):
    keys = jax.random.split(jax.random.fold_in(key, 17), SLOTS)

    def one_board(board_key):
        return jax.random.permutation(board_key, CARDS)[:BOARD_CARDS].astype(jnp.int32)
    return jax.vmap(one_board)(keys)


def draw_board_live(key, part):
    coins = jax.random.randint(jax.random.fold_in(key, 29), (SLOTS,), 0, 2).astype(jnp.int32)
    leading = jnp.arange(SLOTS) % BOARD_DEV == 0
    return jnp.where(leading, 1, coins).astype(jnp.int32)


def place_ends(drawn, key, low, top_value):
    index_at = [jax.random.randint(jax.random.fold_in(key, axis), (), 0, length) for axis, length in enumerate(drawn.shape)]
    main_axis = drawn.shape.index(max(drawn.shape))
    next_to = index_at[:main_axis] + [(index_at[main_axis] + 1) % drawn.shape[main_axis]] + index_at[main_axis + 1:]
    return drawn.at[tuple(index_at)].set(low).at[tuple(next_to)].set(top_value)


def level_of(own_key, dims, shards, low, largest):
    loudness = 1.0
    for position, shards_of in shards:
        steps = jax.random.uniform(jax.random.fold_in(jax.random.fold_in(own_key, 6), position), (shards_of,), jnp.float32, low / len(shards), largest / len(shards))
        loudness = loudness * jnp.repeat(jnp.exp(steps), dims[position] // shards_of).reshape((-1,) + (1,) * (len(dims) - 1 - position))
    return loudness


def scatter_about(stream_key, dims, width, most, kind=jnp.bfloat16):
    values = jax.random.normal(stream_key, dims, jnp.float32) * width
    return jnp.minimum(jnp.maximum(values, -most), most).astype(kind)


def setup_inputs(seed: int = 0) -> dict:
    seeds = jax.random.split(jax.random.key(seed), 8)
    return {
        "root_reach": jnp.clip(jnp.exp(jax.random.uniform(seeds[0], (2, NODES, H), jnp.float32, math.log(0.05), math.log(1.0))), 0.05, 1.0),
        "frontier_value": scatter_about(seeds[1], (2, NODES, H), 10.0, 60.0, jnp.float32),
        "regret_stop": jnp.clip(jnp.exp(math.log(30.0) - 3.4011974 * jax.random.uniform(seeds[2], (SECTIONS, SLOTS, NODES, H), jnp.float32) ** level_of(seeds[2], (SECTIONS, SLOTS, NODES, H), ((0, 8), (1, 4)), -0.2, 0.2)), 1.0, 30.0),
        "regret_go": jnp.clip(jnp.exp(math.log(30.0) - 3.4011974 * jax.random.uniform(seeds[3], (SECTIONS, SLOTS, NODES, H), jnp.float32) ** level_of(seeds[3], (SECTIONS, SLOTS, NODES, H), ((0, 8), (1, 4)), -0.2, 0.2)), 1.0, 30.0),
        "board_live": draw_board_live(jax.random.fold_in(seeds[7], 71), 0),
        "board_cards": draw_board_cards(jax.random.fold_in(seeds[7], 71), 0),
        "hand_rank": place_ends(jax.random.randint(seeds[6], (SLOTS, H), 0, H), jax.random.fold_in(seeds[6], 1), 0, H - 1).astype(jnp.int32),
    }


def free_pairs():
    first, second = np.triu_indices(CARDS, 1)
    first = jnp.asarray(first.astype(np.int32))
    second = jnp.asarray(second.astype(np.int32))
    shared = (first[:, None] == first[None, :]) | (first[:, None] == second[None, :]) | (second[:, None] == first[None, :]) | (second[:, None] == second[None, :])
    return jnp.where(shared, 0.0, 1.0).astype(jnp.bfloat16)


def board_masks(board_cards):
    first, second = np.triu_indices(CARDS, 1)
    first = jnp.asarray(first.astype(np.int32))
    second = jnp.asarray(second.astype(np.int32))
    hits = (board_cards[:, :, None] == first[None, None, :]) | (board_cards[:, :, None] == second[None, None, :])
    return jnp.where(jnp.any(hits, axis=1), 0.0, 1.0).astype(jnp.float32)


def showdown(reach_one, stop_weight, mask_row, rank_row, disjoint):
    leaf_reach = (reach_one * stop_weight).astype(jnp.bfloat16)
    mask_half = mask_row.astype(jnp.bfloat16)
    payoff = jnp.sign(rank_row[:, None] - rank_row[None, :]).astype(jnp.bfloat16) * disjoint * mask_half[:, None] * mask_half[None, :]
    flipped = leaf_reach[::-1].reshape(-1, leaf_reach.shape[-1])
    result = jnp.dot(flipped.astype(jnp.float32), payoff.astype(jnp.float32).T, precision=lax.Precision.HIGHEST)
    return result.reshape(leaf_reach.shape)


def reference(root_reach, frontier_value, regret_stop, regret_go, board_live, board_cards, hand_rank):
    disjoint = free_pairs()
    masks = board_masks(board_cards)
    regret_sum = regret_stop + regret_go
    stop_prob = regret_stop / regret_sum
    go_prob = regret_go / regret_sum
    alive = (board_live > 0).astype(jnp.float32)
    board_total = jnp.sum(alive)
    depth_total = regret_stop.shape[0]
    players = jnp.arange(2)[:, None, None]
    reach_now = root_reach[None] * masks[:, None, None, :]
    leaf_store = []
    for level in range(depth_total):
        acting = players == level % 2
        factor = jnp.where(acting[None], go_prob[level][:, None], 1.0)
        stop_weight = jnp.where(acting[None], stop_prob[level][:, None], 1.0)

        def one_board(items):
            reach_one, weight_one, mask_row, rank_row, alive_one = items
            return lax.cond(alive_one > 0,
                            lambda: showdown(reach_one, weight_one, mask_row, rank_row, disjoint),
                            lambda: jnp.zeros(reach_one.shape, jnp.float32))

        leaf_values = lax.map(one_board, (reach_now, stop_weight, masks, hand_rank, alive))
        leaf_store.append(leaf_values)
        reach_now = reach_now * factor
    value_next = frontier_value[None] * masks[:, None, None, :]
    nexts = [None] * depth_total
    totals = [None] * depth_total
    for level in reversed(range(depth_total)):
        acting = players == level % 2
        factor = jnp.where(acting[None], go_prob[level][:, None], 1.0)
        stop_weight = jnp.where(acting[None], stop_prob[level][:, None], 1.0)
        nexts[level] = value_next
        value_next = stop_weight * leaf_store[level] + factor * value_next
        totals[level] = jnp.sum(alive[:, None, None, None] * value_next, axis=0) / board_total
    stops = []
    goes = []
    for level in range(depth_total):
        acting = players == level % 2
        own_next = jnp.sum(jnp.where(acting[None], nexts[level], 0.0), axis=1)
        own_leaf = jnp.sum(jnp.where(acting[None], leaf_store[level], 0.0), axis=1)
        gap = own_leaf - own_next
        keep_slot = alive[:, None, None] > 0
        stops.append(jnp.where(keep_slot, jnp.maximum(regret_stop[level] + go_prob[level] * gap, 0.0), regret_stop[level]))
        goes.append(jnp.where(keep_slot, jnp.maximum(regret_go[level] - stop_prob[level] * gap, 0.0), regret_go[level]))
    return (jnp.stack(stops), jnp.stack(goes), jnp.stack(totals))
```

```python
import functools

import jax
import jax.numpy as jnp
import numpy as np
from jax import lax
from jax.experimental import pallas as pl
from jax.experimental.pallas import tpu as pltpu
from jax.sharding import PartitionSpec as P

CARDS = 52
LANES = 128
MESH = pl.DeviceIdType.MESH


def pair_tables(hands, width):
    first, second = np.triu_indices(CARDS, 1)
    cards = np.full((8, width), -1, np.int32)
    cards[0, :hands] = first
    cards[1, :hands] = second
    holds = np.zeros((width, LANES), np.float32)
    holds[np.arange(hands), first] = 1.0
    holds[np.arange(hands), second] = 1.0
    left = -holds
    left[:hands, CARDS] = 1.0
    right = holds.T.copy()
    right[CARDS, :hands] = 1.0
    return (
        jnp.asarray(cards),
        jnp.asarray(left, jnp.bfloat16),
        jnp.asarray(right, jnp.bfloat16),
    )


def kernel(
    sizes,
    root_ref,
    frontier_ref,
    stop_ref,
    go_ref,
    live_ref,
    board_ref,
    rank_ref,
    cards_ref,
    left_ref,
    right_ref,
    new_stop_ref,
    new_go_ref,
    value_ref,
    go_send,
    go_recv,
    gap_send,
    gap_recv,
    sum_send,
    sum_recv,
    part_send,
    part_recv,
    free_pairs,
    payoff,
    reach_rows,
    leaf_rows,
    gap_home,
    send1,
    recv1,
    send2,
    recv2,
    send3,
    recv3,
    send4,
    recv4,
):
    depths, groups, boards, nodes, hands, width, chunk = sizes
    me = lax.axis_index("section")
    group = lax.axis_index("board")
    barrier = pltpu.get_barrier_semaphore()
    for step in range(1, depths):
        peer = lax.rem(me + step, depths)
        pl.semaphore_signal(barrier, inc=1, device_id={"section": peer}, device_id_type=MESH)
    for step in range(1, groups):
        peer = lax.rem(group + step, groups)
        pl.semaphore_signal(barrier, inc=1, device_id={"board": peer}, device_id_type=MESH)

    tail = width - LANES
    go_send[:, :, tail:] = jnp.zeros((depths, chunk, LANES), jnp.float32)
    for j in range(boards):
        stop_now = stop_ref[j]
        go_now = go_ref[j]
        go_prob = go_now / (stop_now + go_now)
        for n in range(nodes):
            unit = n * boards + j
            go_send[unit // chunk, unit % chunk : unit % chunk + 1, :hands] = go_prob[n : n + 1]

    pl.semaphore_wait(barrier, depths - 1 + groups - 1)

    def go_copy(target):
        return pltpu.make_async_remote_copy(
            src_ref=go_send.at[target],
            dst_ref=go_recv.at[me],
            send_sem=send1.at[target],
            recv_sem=recv1.at[me],
            device_id={"section": target},
            device_id_type=MESH,
        )

    def go_arrival(source):
        return pltpu.make_async_remote_copy(
            src_ref=go_send.at[source],
            dst_ref=go_recv.at[source],
            send_sem=send1.at[source],
            recv_sem=recv1.at[source],
            device_id={"section": source},
            device_id_type=MESH,
        )

    for step in range(1, depths):
        go_copy(lax.rem(me + step, depths)).start()
    go_recv[me] = go_send[me]

    node = (me * chunk) // boards
    block = lax.rem(me, boards // chunk)
    rank = rank_ref[block].astype(jnp.float32)
    rank = jnp.concatenate(
        [rank, jnp.zeros((chunk, width - hands), jnp.float32)], axis=1
    )
    rank = jnp.concatenate([rank, jnp.zeros((8 - chunk, width), jnp.float32)], axis=0)
    rank_col = jnp.transpose(rank)
    free_pairs[...] = jnp.maximum(
        jnp.dot(left_ref[...], right_ref[...], preferred_element_type=jnp.float32), 0.0
    ).astype(jnp.bfloat16)
    for i in range(chunk):
        for top in range(0, width, LANES):
            diff = rank[i : i + 1, :] - rank_col[top : top + LANES, i : i + 1]
            sign = jnp.clip(diff, -1.0, 1.0).astype(jnp.bfloat16)
            payoff[i, top : top + LANES, :] = sign * free_pairs[top : top + LANES, :]

    lane = lax.broadcasted_iota(jnp.int32, (chunk, width), 1)
    mask = lane < hands
    cards = board_ref[block]
    for m in range(cards.shape[1]):
        card = cards[:, m : m + 1]
        mask = mask & (cards_ref[0:1, :] != card) & (cards_ref[1:2, :] != card)
    mask = jnp.where(mask, 1.0, 0.0)

    pad = jnp.zeros((1, width - hands), jnp.float32)

    def node_row(ref, player):
        return jnp.concatenate([ref[player, pl.ds(node, 1), :], pad], axis=1) * mask

    reach = [node_row(root_ref, p) for p in range(2)]

    for step in range(1, depths):
        go_arrival(lax.rem(me + depths - step, depths)).wait_recv()

    for t in range(depths):
        q = t % 2
        go_t = go_recv[t]
        weighted = [reach[0], reach[1]]
        weighted[q] = reach[q] * (1.0 - go_t)
        for p in range(2):
            for i in range(chunk):
                row = p * depths + t
                reach_rows[i, row : row + 1, :] = weighted[1 - p][i : i + 1]
        reach[q] = reach[q] * go_t
    for i in range(chunk):
        leaf_rows[i] = jnp.dot(
            reach_rows[i].astype(jnp.bfloat16),
            payoff[i],
            preferred_element_type=jnp.float32,
        )

    def gap_copy(target, source):
        return pltpu.make_async_remote_copy(
            src_ref=gap_send.at[target],
            dst_ref=gap_recv.at[source],
            send_sem=send2.at[target],
            recv_sem=recv2.at[source],
            device_id={"section": target},
            device_id_type=MESH,
        )

    def sum_copy(target, source):
        return pltpu.make_async_remote_copy(
            src_ref=sum_send.at[target],
            dst_ref=sum_recv.at[source],
            send_sem=send3.at[target],
            recv_sem=recv3.at[source],
            device_id={"section": target},
            device_id_type=MESH,
        )

    value = [node_row(frontier_ref, p) for p in range(2)]
    alive = [
        jnp.where(live_ref[block * chunk + i] > 0, 1.0, 0.0) for i in range(chunk)
    ]
    for t in reversed(range(depths)):
        q = t % 2
        go_t = go_recv[t]
        leaf = [
            jnp.concatenate(
                [leaf_rows[i, p * depths + t : p * depths + t + 1, :] for i in range(chunk)],
                axis=0,
            )
            * mask
            for p in range(2)
        ]
        gap_send[t] = leaf[q] - value[q]
        value[q] = (1.0 - go_t) * leaf[q] + go_t * value[q]
        value[1 - q] = leaf[1 - q] + value[1 - q]
        for p in range(2):
            total = alive[0] * value[p][0:1]
            for i in range(1, chunk):
                total = total + alive[i] * value[p][i : i + 1]
            sum_send[t, p : p + 1, :] = total

        @pl.when(t != me)
        def _():
            gap_copy(t, me).start()
            sum_copy(t, me).start()

    gap_recv[me] = gap_send[me]
    sum_recv[me] = sum_send[me]

    for step in range(1, depths):
        sum_copy(0, lax.rem(me + depths - step, depths)).wait_recv()
    per_node = boards // chunk
    for n in range(nodes):
        for p in range(2):
            total = sum_recv[n * per_node, p : p + 1, :]
            for extra in range(1, per_node):
                total = total + sum_recv[n * per_node + extra, p : p + 1, :]
            part_send[p, n : n + 1, :] = total
    live_count = jnp.where(live_ref[0] > 0, 1.0, 0.0)
    for j in range(1, boards):
        live_count = live_count + jnp.where(live_ref[j] > 0, 1.0, 0.0)
    part_send[:, :, hands:] = jnp.full((2, nodes, width - hands), 1.0, jnp.float32) * live_count

    def part_copy(target, source):
        return pltpu.make_async_remote_copy(
            src_ref=part_send,
            dst_ref=part_recv.at[source],
            send_sem=send4.at[target],
            recv_sem=recv4.at[source],
            device_id={"board": target},
            device_id_type=MESH,
        )

    for step in range(1, groups):
        part_copy(lax.rem(group + step, groups), group).start()
    part_recv[group] = part_send[...]

    for step in range(1, depths):
        gap_copy(0, lax.rem(me + depths - step, depths)).wait_recv()
    for k in range(depths):
        for i in range(chunk):
            unit = k * chunk + i
            n, j = unit // boards, unit % boards
            gap_home[j, n : n + 1, :] = gap_recv[k, i : i + 1, :]
    for j in range(boards):
        stop_now = stop_ref[j]
        go_now = go_ref[j]
        total = stop_now + go_now
        keep = live_ref[j] > 0
        gap = gap_home[j][:, :hands]
        new_stop = jnp.maximum(stop_now + (go_now / total) * gap, 0.0)
        new_go = jnp.maximum(go_now - (stop_now / total) * gap, 0.0)
        new_stop_ref[j] = jnp.where(keep, new_stop, stop_now)
        new_go_ref[j] = jnp.where(keep, new_go, go_now)

    for step in range(1, groups):
        part_copy(0, lax.rem(group + groups - step, groups)).wait_recv()
    for p in range(2):
        total = part_recv[0, p]
        for b in range(1, groups):
            total = total + part_recv[b, p]
        value_ref[p] = total[:, :hands] / total[:, hands : hands + 1]

    for step in range(1, depths):
        peer = lax.rem(me + step, depths)
        go_copy(peer).wait_send()
        gap_copy(peer, me).wait_send()
        sum_copy(peer, me).wait_send()
    for step in range(1, groups):
        part_copy(lax.rem(group + step, groups), group).wait_send()


def local(depths, groups, root, frontier, regret_stop, regret_go, live, board_cards, rank):
    boards, nodes, hands = regret_stop.shape[1:]
    width = -(-hands // LANES) * LANES
    chunk = nodes * boards // depths
    sizes = (depths, groups, boards, nodes, hands, width, chunk)
    cards, left, right = pair_tables(hands, width)
    vmem = pl.BlockSpec(memory_space=pltpu.VMEM)
    smem = pl.BlockSpec(memory_space=pltpu.SMEM)
    f32 = jnp.float32
    dma = pltpu.SemaphoreType.DMA
    outs = pl.pallas_call(
        functools.partial(kernel, sizes),
        out_shape=(
            jax.ShapeDtypeStruct((boards, nodes, hands), f32),
            jax.ShapeDtypeStruct((boards, nodes, hands), f32),
            jax.ShapeDtypeStruct((2, nodes, hands), f32),
        ),
        in_specs=[vmem] * 4 + [smem] + [vmem] * 5,
        out_specs=(vmem, vmem, vmem),
        scratch_shapes=[
            pltpu.VMEM((depths, chunk, width), f32),
            pltpu.VMEM((depths, chunk, width), f32),
            pltpu.VMEM((depths, chunk, width), f32),
            pltpu.VMEM((depths, chunk, width), f32),
            pltpu.VMEM((depths, 2, width), f32),
            pltpu.VMEM((depths, 2, width), f32),
            pltpu.VMEM((2, nodes, width), f32),
            pltpu.VMEM((groups, 2, nodes, width), f32),
            pltpu.VMEM((width, width), jnp.bfloat16),
            pltpu.VMEM((chunk, width, width), jnp.bfloat16),
            pltpu.VMEM((chunk, 2 * depths, width), f32),
            pltpu.VMEM((chunk, 2 * depths, width), f32),
            pltpu.VMEM((boards, nodes, width), f32),
            dma((depths,)),
            dma((depths,)),
            dma((depths,)),
            dma((depths,)),
            dma((depths,)),
            dma((depths,)),
            dma((groups,)),
            dma((groups,)),
        ],
        compiler_params=pltpu.CompilerParams(
            collective_id=0, has_side_effects=True, vmem_limit_bytes=56 * 1024 * 1024
        ),
    )(
        root,
        frontier,
        regret_stop[0],
        regret_go[0],
        live,
        board_cards.reshape(boards // chunk, chunk, -1),
        rank.reshape(boards // chunk, chunk, hands),
        cards,
        left,
        right,
    )
    return tuple(out[None] for out in outs)


def solution(mesh):
    return jax.shard_map(
        functools.partial(local, mesh.shape["section"], mesh.shape["board"]),
        mesh=mesh,
        in_specs=(
            P(),
            P(),
            P("section", "board", None, None),
            P("section", "board", None, None),
            P("board"),
            P("board", None),
            P("board", None),
        ),
        out_specs=(
            P("section", "board", None, None),
            P("section", "board", None, None),
            P("section", None, None, None),
        ),
        check_vma=False,
    )
```

```python
import functools

import jax
import jax.numpy as jnp
import numpy as np
from jax import lax
from jax.experimental import pallas as pl
from jax.experimental.pallas import tpu as pltpu
from jax.sharding import PartitionSpec as P

CARDS = 52
LANES = 128
MESH = pl.DeviceIdType.MESH


def pair_tables(hands, width):
    first, second = np.triu_indices(CARDS, 1)
    cards = np.full((8, width), -1, np.int32)
    cards[0, :hands] = first
    cards[1, :hands] = second
    holds = np.zeros((width, LANES), np.float32)
    holds[np.arange(hands), first] = 1.0
    holds[np.arange(hands), second] = 1.0
    left = -holds
    left[:hands, CARDS] = 1.0
    right = holds.T.copy()
    right[CARDS, :hands] = 1.0
    return (
        jnp.asarray(cards),
        jnp.asarray(left, jnp.bfloat16),
        jnp.asarray(right, jnp.bfloat16),
    )


def kernel(
    sizes,
    root_hbm,
    frontier_hbm,
    stop_hbm,
    go_hbm,
    live_hbm,
    board_hbm,
    rank_hbm,
    cards_hbm,
    left_hbm,
    right_hbm,
    new_stop_ref,
    new_go_ref,
    value_ref,
    root_ref,
    frontier_ref,
    stop_ref,
    go_ref,
    live_ref,
    board_ref,
    rank_ref,
    cards_ref,
    left_ref,
    right_ref,
    fetch_sem,
    go_send,
    go_recv,
    gap_send,
    gap_recv,
    sum_send,
    sum_recv,
    part_send,
    part_recv,
    free_pairs,
    payoff,
    reach_rows,
    leaf_rows,
    gap_home,
    send1,
    recv1,
    send2,
    recv2,
    send3,
    recv3,
    send4,
    recv4,
):
    depths, groups, boards, nodes, hands, width, chunk = sizes
    me = lax.axis_index("section")
    group = lax.axis_index("board")
    barrier = pltpu.get_barrier_semaphore()
    for step in range(1, depths):
        peer = lax.rem(me + step, depths)
        pl.semaphore_signal(barrier, inc=1, device_id={"section": peer}, device_id_type=MESH)
    for step in range(1, groups):
        peer = lax.rem(group + step, groups)
        pl.semaphore_signal(barrier, inc=1, device_id={"board": peer}, device_id_type=MESH)

    sources = (stop_hbm, go_hbm, rank_hbm, left_hbm, right_hbm)
    sources += (cards_hbm, board_hbm, root_hbm, frontier_hbm, live_hbm)
    places = (stop_ref, go_ref, rank_ref, left_ref, right_ref)
    places += (cards_ref, board_ref, root_ref, frontier_ref, live_ref)
    fetches = [
        pltpu.make_async_copy(source, place, fetch_sem.at[at])
        for at, (source, place) in enumerate(zip(sources, places))
    ]
    for fetch in fetches:
        fetch.start()

    tail = width - LANES
    go_send[:, :, tail:] = jnp.zeros((depths, chunk, LANES), jnp.float32)
    fetches[0].wait()
    fetches[1].wait()
    for j in range(boards):
        stop_now = stop_ref[j]
        go_now = go_ref[j]
        go_prob = go_now / (stop_now + go_now)
        for n in range(nodes):
            unit = n * boards + j
            go_send[unit // chunk, unit % chunk : unit % chunk + 1, :hands] = go_prob[n : n + 1]

    pl.semaphore_wait(barrier, depths - 1 + groups - 1)

    def go_copy(target):
        return pltpu.make_async_remote_copy(
            src_ref=go_send.at[target],
            dst_ref=go_recv.at[me],
            send_sem=send1.at[target],
            recv_sem=recv1.at[me],
            device_id={"section": target},
            device_id_type=MESH,
        )

    def go_arrival(source):
        return pltpu.make_async_remote_copy(
            src_ref=go_send.at[source],
            dst_ref=go_recv.at[source],
            send_sem=send1.at[source],
            recv_sem=recv1.at[source],
            device_id={"section": source},
            device_id_type=MESH,
        )

    for step in range(1, depths):
        go_copy(lax.rem(me + step, depths)).start()
    go_recv[me] = go_send[me]

    for fetch in fetches[2:]:
        fetch.wait()

    node = (me * chunk) // boards
    block = lax.rem(me, boards // chunk)
    rank = rank_ref[block].astype(jnp.float32)
    rank = jnp.concatenate(
        [rank, jnp.zeros((chunk, width - hands), jnp.float32)], axis=1
    )
    rank = jnp.concatenate([rank, jnp.zeros((8 - chunk, width), jnp.float32)], axis=0)
    rank_col = jnp.transpose(rank)
    free_pairs[...] = jnp.maximum(
        jnp.dot(left_ref[...], right_ref[...], preferred_element_type=jnp.float32), 0.0
    ).astype(jnp.bfloat16)
    for i in range(chunk):
        for top in range(0, width, LANES):
            diff = rank[i : i + 1, :] - rank_col[top : top + LANES, i : i + 1]
            sign = jnp.clip(diff, -1.0, 1.0).astype(jnp.bfloat16)
            payoff[i, top : top + LANES, :] = sign * free_pairs[top : top + LANES, :]

    lane = lax.broadcasted_iota(jnp.int32, (chunk, width), 1)
    mask = lane < hands
    cards = board_ref[block]
    for m in range(cards.shape[1]):
        card = cards[:, m : m + 1]
        mask = mask & (cards_ref[0:1, :] != card) & (cards_ref[1:2, :] != card)
    mask = jnp.where(mask, 1.0, 0.0)

    pad = jnp.zeros((1, width - hands), jnp.float32)

    def node_row(ref, player):
        return jnp.concatenate([ref[player, pl.ds(node, 1), :], pad], axis=1) * mask

    reach = [node_row(root_ref, p) for p in range(2)]

    for step in range(1, depths):
        go_arrival(lax.rem(me + depths - step, depths)).wait_recv()

    for t in range(depths):
        q = t % 2
        go_t = go_recv[t]
        weighted = [reach[0], reach[1]]
        weighted[q] = reach[q] * (1.0 - go_t)
        for p in range(2):
            for i in range(chunk):
                row = p * depths + t
                reach_rows[i, row : row + 1, :] = weighted[1 - p][i : i + 1]
        reach[q] = reach[q] * go_t
    for i in range(chunk):
        leaf_rows[i] = jnp.dot(
            reach_rows[i].astype(jnp.bfloat16),
            payoff[i],
            preferred_element_type=jnp.float32,
        )

    def gap_copy(target, source):
        return pltpu.make_async_remote_copy(
            src_ref=gap_send.at[target],
            dst_ref=gap_recv.at[source],
            send_sem=send2.at[target],
            recv_sem=recv2.at[source],
            device_id={"section": target},
            device_id_type=MESH,
        )

    def sum_copy(target, source):
        return pltpu.make_async_remote_copy(
            src_ref=sum_send.at[target],
            dst_ref=sum_recv.at[source],
            send_sem=send3.at[target],
            recv_sem=recv3.at[source],
            device_id={"section": target},
            device_id_type=MESH,
        )

    value = [node_row(frontier_ref, p) for p in range(2)]
    alive = [
        jnp.where(live_ref[block * chunk + i] > 0, 1.0, 0.0) for i in range(chunk)
    ]
    for t in reversed(range(depths)):
        q = t % 2
        go_t = go_recv[t]
        leaf = [
            jnp.concatenate(
                [leaf_rows[i, p * depths + t : p * depths + t + 1, :] for i in range(chunk)],
                axis=0,
            )
            * mask
            for p in range(2)
        ]
        gap_send[t] = leaf[q] - value[q]
        value[q] = (1.0 - go_t) * leaf[q] + go_t * value[q]
        value[1 - q] = leaf[1 - q] + value[1 - q]
        for p in range(2):
            total = alive[0] * value[p][0:1]
            for i in range(1, chunk):
                total = total + alive[i] * value[p][i : i + 1]
            sum_send[t, p : p + 1, :] = total

        @pl.when(t != me)
        def _():
            sum_copy(t, me).start()

    for step in range(1, depths):
        gap_copy(lax.rem(me + step, depths), me).start()
    gap_recv[me] = gap_send[me]
    sum_recv[me] = sum_send[me]

    for step in range(1, depths):
        sum_copy(0, lax.rem(me + depths - step, depths)).wait_recv()
    per_node = boards // chunk
    for n in range(nodes):
        for p in range(2):
            total = sum_recv[n * per_node, p : p + 1, :]
            for extra in range(1, per_node):
                total = total + sum_recv[n * per_node + extra, p : p + 1, :]
            part_send[p, n : n + 1, :] = total
    live_count = jnp.where(live_ref[0] > 0, 1.0, 0.0)
    for j in range(1, boards):
        live_count = live_count + jnp.where(live_ref[j] > 0, 1.0, 0.0)
    part_send[:, :, hands:] = jnp.full((2, nodes, width - hands), 1.0, jnp.float32) * live_count

    def part_copy(target, source):
        return pltpu.make_async_remote_copy(
            src_ref=part_send,
            dst_ref=part_recv.at[source],
            send_sem=send4.at[target],
            recv_sem=recv4.at[source],
            device_id={"board": target},
            device_id_type=MESH,
        )

    for step in range(1, groups):
        part_copy(lax.rem(group + step, groups), group).start()
    part_recv[group] = part_send[...]

    for step in range(1, depths):
        gap_copy(0, lax.rem(me + depths - step, depths)).wait_recv()
    for k in range(depths):
        for i in range(chunk):
            unit = k * chunk + i
            n, j = unit // boards, unit % boards
            gap_home[j, n : n + 1, :] = gap_recv[k, i : i + 1, :]
    for j in range(boards):
        stop_now = stop_ref[j]
        go_now = go_ref[j]
        total = stop_now + go_now
        keep = live_ref[j] > 0
        gap = gap_home[j][:, :hands]
        new_stop = jnp.maximum(stop_now + (go_now / total) * gap, 0.0)
        new_go = jnp.maximum(go_now - (stop_now / total) * gap, 0.0)
        new_stop_ref[j] = jnp.where(keep, new_stop, stop_now)
        new_go_ref[j] = jnp.where(keep, new_go, go_now)

    for step in range(1, groups):
        part_copy(0, lax.rem(group + groups - step, groups)).wait_recv()
    for p in range(2):
        total = part_recv[0, p]
        for b in range(1, groups):
            total = total + part_recv[b, p]
        value_ref[p] = total[:, :hands] / total[:, hands : hands + 1]

    for step in range(1, depths):
        peer = lax.rem(me + step, depths)
        go_copy(peer).wait_send()
        gap_copy(peer, me).wait_send()
        sum_copy(peer, me).wait_send()
    for step in range(1, groups):
        part_copy(lax.rem(group + step, groups), group).wait_send()


def local(depths, groups, root, frontier, regret_stop, regret_go, live, board_cards, rank):
    boards, nodes, hands = regret_stop.shape[1:]
    width = -(-hands // LANES) * LANES
    chunk = nodes * boards // depths
    sizes = (depths, groups, boards, nodes, hands, width, chunk)
    cards, left, right = pair_tables(hands, width)
    vmem = pl.BlockSpec(memory_space=pltpu.VMEM)
    hbm = pl.BlockSpec(memory_space=pltpu.HBM)
    f32 = jnp.float32
    dma = pltpu.SemaphoreType.DMA
    operands = (
        root,
        frontier,
        regret_stop[0],
        regret_go[0],
        live,
        board_cards.reshape(boards // chunk, chunk, -1),
        rank.reshape(boards // chunk, chunk, hands),
        cards,
        left,
        right,
    )
    outs = pl.pallas_call(
        functools.partial(kernel, sizes),
        out_shape=(
            jax.ShapeDtypeStruct((boards, nodes, hands), f32),
            jax.ShapeDtypeStruct((boards, nodes, hands), f32),
            jax.ShapeDtypeStruct((2, nodes, hands), f32),
        ),
        in_specs=[hbm] * 10,
        out_specs=(vmem, vmem, vmem),
        scratch_shapes=[
            pltpu.VMEM((2, nodes, hands), f32),
            pltpu.VMEM((2, nodes, hands), f32),
            pltpu.VMEM((boards, nodes, hands), f32),
            pltpu.VMEM((boards, nodes, hands), f32),
            pltpu.SMEM((boards,), jnp.int32),
            pltpu.VMEM((boards // chunk, chunk, board_cards.shape[1]), jnp.int32),
            pltpu.VMEM((boards // chunk, chunk, hands), jnp.int32),
            pltpu.VMEM(cards.shape, cards.dtype),
            pltpu.VMEM(left.shape, left.dtype),
            pltpu.VMEM(right.shape, right.dtype),
            dma((10,)),
            pltpu.VMEM((depths, chunk, width), f32),
            pltpu.VMEM((depths, chunk, width), f32),
            pltpu.VMEM((depths, chunk, width), f32),
            pltpu.VMEM((depths, chunk, width), f32),
            pltpu.VMEM((depths, 2, width), f32),
            pltpu.VMEM((depths, 2, width), f32),
            pltpu.VMEM((2, nodes, width), f32),
            pltpu.VMEM((groups, 2, nodes, width), f32),
            pltpu.VMEM((width, width), jnp.bfloat16),
            pltpu.VMEM((chunk, width, width), jnp.bfloat16),
            pltpu.VMEM((chunk, 2 * depths, width), f32),
            pltpu.VMEM((chunk, 2 * depths, width), f32),
            pltpu.VMEM((boards, nodes, width), f32),
            dma((depths,)),
            dma((depths,)),
            dma((depths,)),
            dma((depths,)),
            dma((depths,)),
            dma((depths,)),
            dma((groups,)),
            dma((groups,)),
        ],
        compiler_params=pltpu.CompilerParams(
            collective_id=0, has_side_effects=True, vmem_limit_bytes=36 * 1024 * 1024
        ),
    )(*(pltpu.with_memory_space_constraint(operand, pltpu.HBM) for operand in operands))
    return tuple(out[None] for out in outs)


def solution(mesh):
    return jax.shard_map(
        functools.partial(local, mesh.shape["section"], mesh.shape["board"]),
        mesh=mesh,
        in_specs=(
            P(),
            P(),
            P("section", "board", None, None),
            P("section", "board", None, None),
            P("board"),
            P("board", None),
            P("board", None),
        ),
        out_specs=(
            P("section", "board", None, None),
            P("section", "board", None, None),
            P("section", None, None, None),
        ),
        check_vma=False,
    )
```

```python
import functools

import jax
import jax.numpy as jnp
import numpy as np
from jax import lax
from jax.experimental import pallas as pl
from jax.experimental.pallas import tpu as pltpu
from jax.sharding import PartitionSpec as P

CARDS = 52
LANES = 128
MESH = pl.DeviceIdType.MESH


def pair_tables(hands, width):
    first, second = np.triu_indices(CARDS, 1)
    cards = np.full((8, width), -1, np.int32)
    cards[0, :hands] = first
    cards[1, :hands] = second
    holds = np.zeros((width, LANES), np.float32)
    holds[np.arange(hands), first] = 1.0
    holds[np.arange(hands), second] = 1.0
    left = -holds
    left[:hands, CARDS] = 1.0
    right = holds.T.copy()
    right[CARDS, :hands] = 1.0
    return (
        jnp.asarray(cards),
        jnp.asarray(left, jnp.bfloat16),
        jnp.asarray(right, jnp.bfloat16),
    )


def near_first(count):
    return sorted(range(1, count), key=lambda step: (min(step, count - step), step))


def kernel(
    sizes,
    root_hbm,
    frontier_hbm,
    stop_hbm,
    go_hbm,
    live_hbm,
    board_hbm,
    rank_hbm,
    cards_hbm,
    left_hbm,
    right_hbm,
    new_stop_ref,
    new_go_ref,
    value_ref,
    root_ref,
    frontier_ref,
    stop_ref,
    go_ref,
    live_ref,
    board_ref,
    rank_ref,
    cards_ref,
    left_ref,
    right_ref,
    fetch_sem,
    go_send,
    go_recv,
    gap_send,
    gap_recv,
    sum_send,
    sum_recv,
    free_pairs,
    payoff,
    reach_rows,
    leaf_rows,
    gap_home,
    send1,
    recv1,
    send2,
    recv2,
    send3,
    recv3,
    send4,
    recv4,
):
    depths, groups, boards, nodes, hands, width, chunk = sizes
    me = lax.axis_index("section")
    group = lax.axis_index("board")
    barrier = pltpu.get_barrier_semaphore()
    for step in range(1, depths):
        peer = lax.rem(me + step, depths)
        pl.semaphore_signal(barrier, inc=1, device_id={"section": peer}, device_id_type=MESH)
    for step in range(1, groups):
        peer = lax.rem(group + step, groups)
        pl.semaphore_signal(barrier, inc=1, device_id={"board": peer}, device_id_type=MESH)

    sources = (stop_hbm, go_hbm, rank_hbm, left_hbm, right_hbm)
    sources += (cards_hbm, board_hbm, root_hbm, frontier_hbm, live_hbm)
    places = (stop_ref, go_ref, rank_ref, left_ref, right_ref)
    places += (cards_ref, board_ref, root_ref, frontier_ref, live_ref)
    fetches = [
        pltpu.make_async_copy(source, place, fetch_sem.at[at])
        for at, (source, place) in enumerate(zip(sources, places))
    ]
    for fetch in fetches:
        fetch.start()

    tail = width - LANES
    go_send[:, :, tail:] = jnp.zeros((depths, chunk, LANES), jnp.float32)
    fetches[0].wait()
    fetches[1].wait()
    for j in range(boards):
        stop_now = stop_ref[j]
        go_now = go_ref[j]
        go_prob = go_now / (stop_now + go_now)
        for n in range(nodes):
            unit = n * boards + j
            go_send[unit // chunk, unit % chunk : unit % chunk + 1, :hands] = go_prob[n : n + 1]

    pl.semaphore_wait(barrier, depths - 1 + groups - 1)

    def go_copy(target):
        return pltpu.make_async_remote_copy(
            src_ref=go_send.at[target],
            dst_ref=go_recv.at[me],
            send_sem=send1.at[target],
            recv_sem=recv1.at[me],
            device_id={"section": target},
            device_id_type=MESH,
        )

    def go_arrival(source):
        return pltpu.make_async_remote_copy(
            src_ref=go_send.at[source],
            dst_ref=go_recv.at[source],
            send_sem=send1.at[source],
            recv_sem=recv1.at[source],
            device_id={"section": source},
            device_id_type=MESH,
        )

    for step in reversed(near_first(depths)):
        go_copy(lax.rem(me + step, depths)).start()
    go_recv[me] = go_send[me]

    for fetch in fetches[2:]:
        fetch.wait()

    node = (me * chunk) // boards
    block = lax.rem(me, boards // chunk)
    rank = rank_ref[block].astype(jnp.float32)
    rank = jnp.concatenate(
        [rank, jnp.zeros((chunk, width - hands), jnp.float32)], axis=1
    )
    rank = jnp.concatenate([rank, jnp.zeros((8 - chunk, width), jnp.float32)], axis=0)
    rank_col = jnp.transpose(rank)
    pairs = jnp.maximum(
        jnp.dot(left_ref[...], right_ref[...], preferred_element_type=jnp.float32), 0.0
    ).astype(jnp.bfloat16)
    free_pairs[0] = pairs
    free_pairs[1] = -pairs
    for i in range(chunk):
        for top in range(0, width, LANES):
            diff = rank[i : i + 1, :] - rank_col[top : top + LANES, i : i + 1]
            bounded = jnp.maximum(diff.astype(jnp.bfloat16), free_pairs[1, top : top + LANES, :])
            payoff[i, top : top + LANES, :] = jnp.minimum(
                bounded, free_pairs[0, top : top + LANES, :]
            )

    lane = lax.broadcasted_iota(jnp.int32, (chunk, width), 1)
    mask = lane < hands
    cards = board_ref[block]
    for m in range(cards.shape[1]):
        card = cards[:, m : m + 1]
        mask = mask & (cards_ref[0:1, :] != card) & (cards_ref[1:2, :] != card)
    mask = jnp.where(mask, 1.0, 0.0)

    pad = jnp.zeros((1, width - hands), jnp.float32)

    def node_row(ref, player):
        return jnp.concatenate([ref[player, pl.ds(node, 1), :], pad], axis=1) * mask

    reach = [node_row(root_ref, p) for p in range(2)]

    for step in range(1, depths):
        go_arrival(lax.rem(me + depths - step, depths)).wait_recv()

    for t in range(depths):
        q = t % 2
        go_t = go_recv[t]
        weighted = [reach[0], reach[1]]
        weighted[q] = reach[q] * (1.0 - go_t)
        for p in range(2):
            for i in range(chunk):
                row = p * depths + t
                reach_rows[i, row : row + 1, :] = weighted[1 - p][i : i + 1]
        reach[q] = reach[q] * go_t
    for i in range(chunk):
        leaf_rows[i] = jnp.dot(
            reach_rows[i].astype(jnp.bfloat16),
            payoff[i],
            preferred_element_type=jnp.float32,
        )

    def gap_copy(target, source):
        return pltpu.make_async_remote_copy(
            src_ref=gap_send.at[target],
            dst_ref=gap_recv.at[source],
            send_sem=send2.at[target],
            recv_sem=recv2.at[source],
            device_id={"section": target},
            device_id_type=MESH,
        )

    def sum_copy(target, source):
        return pltpu.make_async_remote_copy(
            src_ref=sum_send.at[target],
            dst_ref=sum_recv.at[group, source],
            send_sem=send3.at[target],
            recv_sem=recv3.at[source],
            device_id={"section": target},
            device_id_type=MESH,
        )

    value = [node_row(frontier_ref, p) for p in range(2)]
    alive = [
        jnp.where(live_ref[block * chunk + i] > 0, 1.0, 0.0) for i in range(chunk)
    ]
    live_here = alive[0]
    for i in range(1, chunk):
        live_here = live_here + alive[i]
    row_lane = lax.broadcasted_iota(jnp.int32, (1, width), 1)
    for t in reversed(range(depths)):
        q = t % 2
        go_t = go_recv[t]
        leaf = [
            jnp.concatenate(
                [leaf_rows[i, p * depths + t : p * depths + t + 1, :] for i in range(chunk)],
                axis=0,
            )
            * mask
            for p in range(2)
        ]
        gap_send[t] = leaf[q] - value[q]
        value[q] = (1.0 - go_t) * leaf[q] + go_t * value[q]
        value[1 - q] = leaf[1 - q] + value[1 - q]
        for p in range(2):
            total = alive[0] * value[p][0:1]
            for i in range(1, chunk):
                total = total + alive[i] * value[p][i : i + 1]
            sum_send[t, p : p + 1, :] = jnp.where(row_lane < hands, total, live_here)

        @pl.when(t != me)
        def _():
            sum_copy(t, me).start()

    for step in reversed(near_first(depths)):
        gap_copy(lax.rem(me + step, depths), me).start()
    sum_recv[group, me] = sum_send[me]
    gap_recv[me] = gap_send[me]

    def part_copy(target, at, source, node_source):
        return pltpu.make_async_remote_copy(
            src_ref=sum_recv.at[source, node_source],
            dst_ref=sum_recv.at[source, node_source],
            send_sem=send4.at[target, node_source],
            recv_sem=recv4.at[at, node_source],
            device_id={"board": target},
            device_id_type=MESH,
        )

    for step in [0] + near_first(depths):
        source = lax.rem(me + step, depths)
        if step:
            sum_copy(0, source).wait_recv()
        for hop in range(1, groups):
            part_copy(lax.rem(group + hop, groups), group, group, source).start()

    for step in range(1, depths):
        gap_copy(0, lax.rem(me + depths - step, depths)).wait_recv()
    for k in range(depths):
        for i in range(chunk):
            unit = k * chunk + i
            n, j = unit // boards, unit % boards
            gap_home[j, n : n + 1, :] = gap_recv[k, i : i + 1, :]
    for j in range(boards):
        stop_now = stop_ref[j]
        go_now = go_ref[j]
        total = stop_now + go_now
        keep = live_ref[j] > 0
        gap = gap_home[j][:, :hands]
        new_stop = jnp.maximum(stop_now + (go_now / total) * gap, 0.0)
        new_go = jnp.maximum(go_now - (stop_now / total) * gap, 0.0)
        new_stop_ref[j] = jnp.where(keep, new_stop, stop_now)
        new_go_ref[j] = jnp.where(keep, new_go, go_now)

    for step in range(1, groups):
        source = lax.rem(group + step, groups)
        for k in range(depths):
            part_copy(source, source, source, k).wait_recv()
    per_node = boards // chunk
    for n in range(nodes):
        total = jnp.zeros((2, width), jnp.float32)
        for b in range(groups):
            for k in range(n * per_node, (n + 1) * per_node):
                total = total + sum_recv[b, k]
        result = total[:, :hands] / total[:, hands : hands + 1]
        for p in range(2):
            value_ref[p, n : n + 1, :] = result[p : p + 1]

    for step in range(1, depths):
        peer = lax.rem(me + step, depths)
        go_copy(peer).wait_send()
        gap_copy(peer, me).wait_send()
        sum_copy(peer, me).wait_send()
    for step in range(1, groups):
        target = lax.rem(group + step, groups)
        for k in range(depths):
            part_copy(target, group, group, k).wait_send()


def write_out(*refs):
    sources, places, sem = refs[:3], refs[3:6], refs[6]
    copies = [
        pltpu.make_async_copy(source, place, sem.at[at])
        for at, (source, place) in enumerate(zip(sources, places))
    ]
    for copy in copies:
        copy.start()
    for copy in copies:
        copy.wait()


def local(depths, groups, root, frontier, regret_stop, regret_go, live, board_cards, rank):
    boards, nodes, hands = regret_stop.shape[1:]
    width = -(-hands // LANES) * LANES
    chunk = nodes * boards // depths
    sizes = (depths, groups, boards, nodes, hands, width, chunk)
    cards, left, right = pair_tables(hands, width)
    vmem = pl.BlockSpec(memory_space=pltpu.VMEM)
    hbm = pl.BlockSpec(memory_space=pltpu.HBM)
    f32 = jnp.float32
    dma = pltpu.SemaphoreType.DMA
    operands = (
        root,
        frontier,
        regret_stop[0],
        regret_go[0],
        live,
        board_cards.reshape(boards // chunk, chunk, -1),
        rank.reshape(boards // chunk, chunk, hands),
        cards,
        left,
        right,
    )
    outs = pl.pallas_call(
        functools.partial(kernel, sizes),
        out_shape=(
            jax.ShapeDtypeStruct((boards, nodes, hands), f32),
            jax.ShapeDtypeStruct((boards, nodes, hands), f32),
            jax.ShapeDtypeStruct((2, nodes, hands), f32),
        ),
        in_specs=[hbm] * 10,
        out_specs=(vmem, vmem, vmem),
        scratch_shapes=[
            pltpu.VMEM((2, nodes, hands), f32),
            pltpu.VMEM((2, nodes, hands), f32),
            pltpu.VMEM((boards, nodes, hands), f32),
            pltpu.VMEM((boards, nodes, hands), f32),
            pltpu.SMEM((boards,), jnp.int32),
            pltpu.VMEM((boards // chunk, chunk, board_cards.shape[1]), jnp.int32),
            pltpu.VMEM((boards // chunk, chunk, hands), jnp.int32),
            pltpu.VMEM(cards.shape, cards.dtype),
            pltpu.VMEM(left.shape, left.dtype),
            pltpu.VMEM(right.shape, right.dtype),
            dma((10,)),
            pltpu.VMEM((depths, chunk, width), f32),
            pltpu.VMEM((depths, chunk, width), f32),
            pltpu.VMEM((depths, chunk, width), f32),
            pltpu.VMEM((depths, chunk, width), f32),
            pltpu.VMEM((depths, 2, width), f32),
            pltpu.VMEM((groups, depths, 2, width), f32),
            pltpu.VMEM((2, width, width), jnp.bfloat16),
            pltpu.VMEM((chunk, width, width), jnp.bfloat16),
            pltpu.VMEM((chunk, 2 * depths, width), f32),
            pltpu.VMEM((chunk, 2 * depths, width), f32),
            pltpu.VMEM((boards, nodes, width), f32),
            dma((depths,)),
            dma((depths,)),
            dma((depths,)),
            dma((depths,)),
            dma((depths,)),
            dma((depths,)),
            dma((groups, depths)),
            dma((groups, depths)),
        ],
        compiler_params=pltpu.CompilerParams(
            collective_id=0, has_side_effects=True, vmem_limit_bytes=42 * 1024 * 1024
        ),
    )(*(pltpu.with_memory_space_constraint(operand, pltpu.HBM) for operand in operands))
    whole = [out[None] for out in outs]
    return pl.pallas_call(
        write_out,
        out_shape=tuple(jax.ShapeDtypeStruct(out.shape, f32) for out in whole),
        in_specs=[pl.BlockSpec(memory_space=pl.ANY)] * 3,
        out_specs=tuple(pl.BlockSpec(memory_space=pl.ANY) for _ in whole),
        scratch_shapes=[dma((3,))],
        compiler_params=pltpu.CompilerParams(vmem_limit_bytes=1024 * 1024),
    )(*whole)


def solution(mesh):
    return jax.shard_map(
        functools.partial(local, mesh.shape["section"], mesh.shape["board"]),
        mesh=mesh,
        in_specs=(
            P(),
            P(),
            P("section", "board", None, None),
            P("section", "board", None, None),
            P("board"),
            P("board", None),
            P("board", None),
        ),
        out_specs=(
            P("section", "board", None, None),
            P("section", "board", None, None),
            P("section", None, None, None),
        ),
        check_vma=False,
    )
```

```python
import functools

import jax
import jax.numpy as jnp
import numpy as np
from jax import lax
from jax.experimental import pallas as pl
from jax.experimental.pallas import tpu as pltpu
from jax.sharding import PartitionSpec as P

CARDS = 52
LANES = 128
MESH = pl.DeviceIdType.MESH


def pair_tables(hands, width):
    first, second = np.triu_indices(CARDS, 1)
    cards = np.full((8, width), -1, np.int32)
    cards[0, :hands] = first
    cards[1, :hands] = second
    holds = np.zeros((width, LANES), np.float32)
    holds[np.arange(hands), first] = 1.0
    holds[np.arange(hands), second] = 1.0
    left = -holds
    left[:hands, CARDS] = 1.0
    right = holds.T.copy()
    right[CARDS, :hands] = 1.0
    return (
        jnp.asarray(cards),
        jnp.asarray(left, jnp.bfloat16),
        jnp.asarray(right, jnp.bfloat16),
    )


def near_first(count):
    return sorted(range(1, count), key=lambda step: (min(step, count - step), step))


def kernel(
    sizes,
    root_hbm,
    frontier_hbm,
    stop_hbm,
    go_hbm,
    live_hbm,
    board_hbm,
    rank_hbm,
    cards_hbm,
    left_hbm,
    right_hbm,
    new_stop_ref,
    new_go_ref,
    value_ref,
    root_ref,
    frontier_ref,
    stop_ref,
    go_ref,
    live_ref,
    board_ref,
    rank_ref,
    cards_ref,
    left_ref,
    right_ref,
    fetch_sem,
    go_send,
    go_recv,
    gap_send,
    gap_recv,
    sum_send,
    sum_recv,
    free_pairs,
    payoff,
    reach_rows,
    leaf_rows,
    gap_home,
    prob_home,
    send1,
    recv1,
    send2,
    recv2,
    send3,
    recv3,
    send4,
    recv4,
):
    depths, groups, boards, nodes, hands, width, chunk = sizes
    me = lax.axis_index("section")
    group = lax.axis_index("board")
    barrier = pltpu.get_barrier_semaphore()
    for step in range(1, depths):
        peer = lax.rem(me + step, depths)
        pl.semaphore_signal(barrier, inc=1, device_id={"section": peer}, device_id_type=MESH)
    for step in range(1, groups):
        peer = lax.rem(group + step, groups)
        pl.semaphore_signal(barrier, inc=1, device_id={"board": peer}, device_id_type=MESH)

    sources = (stop_hbm, go_hbm, rank_hbm, left_hbm, right_hbm)
    sources += (cards_hbm, board_hbm, root_hbm, frontier_hbm, live_hbm)
    places = (stop_ref, go_ref, rank_ref, left_ref, right_ref)
    places += (cards_ref, board_ref, root_ref, frontier_ref, live_ref)
    fetches = [
        pltpu.make_async_copy(source, place, fetch_sem.at[at])
        for at, (source, place) in enumerate(zip(sources, places))
    ]
    for fetch in fetches:
        fetch.start()

    tail = width - LANES
    go_send[:, :, tail:] = jnp.zeros((depths, chunk, LANES), jnp.float32)
    fetches[0].wait()
    fetches[1].wait()
    for j in range(boards):
        stop_now = stop_ref[j]
        go_now = go_ref[j]
        go_prob = go_now / (stop_now + go_now)
        prob_home[j] = go_prob
        for n in range(nodes):
            unit = n * boards + j
            go_send[unit // chunk, unit % chunk : unit % chunk + 1, :hands] = go_prob[n : n + 1]

    pl.semaphore_wait(barrier, depths - 1 + groups - 1)

    def go_copy(target):
        return pltpu.make_async_remote_copy(
            src_ref=go_send.at[target],
            dst_ref=go_recv.at[me],
            send_sem=send1.at[target],
            recv_sem=recv1.at[me],
            device_id={"section": target},
            device_id_type=MESH,
        )

    def go_arrival(source):
        return pltpu.make_async_remote_copy(
            src_ref=go_send.at[source],
            dst_ref=go_recv.at[source],
            send_sem=send1.at[source],
            recv_sem=recv1.at[source],
            device_id={"section": source},
            device_id_type=MESH,
        )

    for step in reversed(near_first(depths)):
        go_copy(lax.rem(me + step, depths)).start()
    go_recv[me] = go_send[me]

    for fetch in fetches[2:]:
        fetch.wait()

    node = (me * chunk) // boards
    block = lax.rem(me, boards // chunk)
    rank = rank_ref[block].astype(jnp.float32)
    rank = jnp.concatenate(
        [rank, jnp.zeros((chunk, width - hands), jnp.float32)], axis=1
    )
    rank = jnp.concatenate([rank, jnp.zeros((8 - chunk, width), jnp.float32)], axis=0)
    rank_col = jnp.transpose(rank)
    pairs = jnp.maximum(
        jnp.dot(left_ref[...], right_ref[...], preferred_element_type=jnp.float32), 0.0
    ).astype(jnp.bfloat16)
    free_pairs[0] = pairs
    free_pairs[1] = -pairs
    for i in range(chunk):
        for top in range(0, width, LANES):
            diff = rank[i : i + 1, :] - rank_col[top : top + LANES, i : i + 1]
            bounded = jnp.maximum(diff.astype(jnp.bfloat16), free_pairs[1, top : top + LANES, :])
            payoff[i, top : top + LANES, :] = jnp.minimum(
                bounded, free_pairs[0, top : top + LANES, :]
            )

    lane = lax.broadcasted_iota(jnp.int32, (chunk, width), 1)
    mask = lane < hands
    cards = board_ref[block]
    for m in range(cards.shape[1]):
        card = cards[:, m : m + 1]
        mask = mask & (cards_ref[0:1, :] != card) & (cards_ref[1:2, :] != card)
    mask = jnp.where(mask, 1.0, 0.0)

    pad = jnp.zeros((1, width - hands), jnp.float32)

    def node_row(ref, player):
        return jnp.concatenate([ref[player, pl.ds(node, 1), :], pad], axis=1) * mask

    reach = [node_row(root_ref, p) for p in range(2)]

    for t in range(depths):
        q = t % 2

        @pl.when(t != me)
        def _():
            go_arrival(t).wait_recv()

        go_t = go_recv[t]
        weighted = [reach[0], reach[1]]
        weighted[q] = reach[q] * (1.0 - go_t)
        for p in range(2):
            for i in range(chunk):
                row = p * depths + t
                reach_rows[i, row : row + 1, :] = weighted[1 - p][i : i + 1]
        reach[q] = reach[q] * go_t
    for i in range(chunk):
        leaf_rows[i] = jnp.dot(
            reach_rows[i].astype(jnp.bfloat16),
            payoff[i],
            preferred_element_type=jnp.float32,
        )

    def gap_copy(target, source):
        return pltpu.make_async_remote_copy(
            src_ref=gap_send.at[target],
            dst_ref=gap_recv.at[source],
            send_sem=send2.at[target],
            recv_sem=recv2.at[source],
            device_id={"section": target},
            device_id_type=MESH,
        )

    def sum_copy(target, source):
        return pltpu.make_async_remote_copy(
            src_ref=sum_send.at[target],
            dst_ref=sum_recv.at[group, source],
            send_sem=send3.at[target],
            recv_sem=recv3.at[source],
            device_id={"section": target},
            device_id_type=MESH,
        )

    value = [node_row(frontier_ref, p) for p in range(2)]
    alive = [
        jnp.where(live_ref[block * chunk + i] > 0, 1.0, 0.0) for i in range(chunk)
    ]
    live_here = alive[0]
    for i in range(1, chunk):
        live_here = live_here + alive[i]
    row_lane = lax.broadcasted_iota(jnp.int32, (1, width), 1)
    for t in reversed(range(depths)):
        q = t % 2
        go_t = go_recv[t]
        leaf = [
            jnp.concatenate(
                [leaf_rows[i, p * depths + t : p * depths + t + 1, :] for i in range(chunk)],
                axis=0,
            )
            * mask
            for p in range(2)
        ]
        gap_send[t] = leaf[q] - value[q]
        value[q] = (1.0 - go_t) * leaf[q] + go_t * value[q]
        value[1 - q] = leaf[1 - q] + value[1 - q]
        for p in range(2):
            total = alive[0] * value[p][0:1]
            for i in range(1, chunk):
                total = total + alive[i] * value[p][i : i + 1]
            sum_send[t, p : p + 1, :] = jnp.where(row_lane < hands, total, live_here)

        @pl.when(t != me)
        def _():
            sum_copy(t, me).start()

    sum_recv[group, me] = sum_send[me]
    gap_recv[me] = gap_send[me]

    def part_copy(target, at, source, node_source):
        return pltpu.make_async_remote_copy(
            src_ref=sum_recv.at[source, node_source],
            dst_ref=sum_recv.at[source, node_source],
            send_sem=send4.at[target, node_source],
            recv_sem=recv4.at[at, node_source],
            device_id={"board": target},
            device_id_type=MESH,
        )

    for step in [0] + near_first(depths):
        source = lax.rem(me + step, depths)
        if step:
            sum_copy(0, source).wait_recv()
        for hop in range(1, groups):
            part_copy(lax.rem(group + hop, groups), group, group, source).start()

    for step in reversed(near_first(depths)):
        gap_copy(lax.rem(me + step, depths), me).start()

    for step in range(1, depths):
        gap_copy(0, lax.rem(me + depths - step, depths)).wait_recv()
    for k in range(depths):
        for i in range(chunk):
            unit = k * chunk + i
            n, j = unit // boards, unit % boards
            gap_home[j, n : n + 1, :] = gap_recv[k, i : i + 1, :]
    for j in range(boards):
        stop_now = stop_ref[j]
        go_now = go_ref[j]
        go_prob = prob_home[j]
        keep = live_ref[j] > 0
        gap = gap_home[j][:, :hands]
        new_stop = jnp.maximum(stop_now + go_prob * gap, 0.0)
        new_go = jnp.maximum(go_now - (1.0 - go_prob) * gap, 0.0)
        new_stop_ref[j] = jnp.where(keep, new_stop, stop_now)
        new_go_ref[j] = jnp.where(keep, new_go, go_now)

    for step in range(1, groups):
        source = lax.rem(group + step, groups)
        for k in range(depths):
            part_copy(source, source, source, k).wait_recv()
    per_node = boards // chunk
    for n in range(nodes):
        total = jnp.zeros((2, width), jnp.float32)
        for b in range(groups):
            for k in range(n * per_node, (n + 1) * per_node):
                total = total + sum_recv[b, k]
        result = total[:, :hands] / total[:, hands : hands + 1]
        for p in range(2):
            value_ref[p, n : n + 1, :] = result[p : p + 1]

    for step in range(1, depths):
        peer = lax.rem(me + step, depths)
        go_copy(peer).wait_send()
        gap_copy(peer, me).wait_send()
        sum_copy(peer, me).wait_send()
    for step in range(1, groups):
        target = lax.rem(group + step, groups)
        for k in range(depths):
            part_copy(target, group, group, k).wait_send()


def write_out(*refs):
    sources, places, sem = refs[:3], refs[3:6], refs[6]
    copies = [
        pltpu.make_async_copy(source, place, sem.at[at])
        for at, (source, place) in enumerate(zip(sources, places))
    ]
    for copy in copies:
        copy.start()
    for copy in copies:
        copy.wait()


def local(depths, groups, root, frontier, regret_stop, regret_go, live, board_cards, rank):
    boards, nodes, hands = regret_stop.shape[1:]
    width = -(-hands // LANES) * LANES
    chunk = nodes * boards // depths
    sizes = (depths, groups, boards, nodes, hands, width, chunk)
    cards, left, right = pair_tables(hands, width)
    vmem = pl.BlockSpec(memory_space=pltpu.VMEM)
    hbm = pl.BlockSpec(memory_space=pltpu.HBM)
    f32 = jnp.float32
    dma = pltpu.SemaphoreType.DMA
    operands = (
        root,
        frontier,
        regret_stop[0],
        regret_go[0],
        live,
        board_cards.reshape(boards // chunk, chunk, -1),
        rank.reshape(boards // chunk, chunk, hands),
        cards,
        left,
        right,
    )
    outs = pl.pallas_call(
        functools.partial(kernel, sizes),
        out_shape=(
            jax.ShapeDtypeStruct((boards, nodes, hands), f32),
            jax.ShapeDtypeStruct((boards, nodes, hands), f32),
            jax.ShapeDtypeStruct((2, nodes, hands), f32),
        ),
        in_specs=[hbm] * 10,
        out_specs=(vmem, vmem, vmem),
        scratch_shapes=[
            pltpu.VMEM((2, nodes, hands), f32),
            pltpu.VMEM((2, nodes, hands), f32),
            pltpu.VMEM((boards, nodes, hands), f32),
            pltpu.VMEM((boards, nodes, hands), f32),
            pltpu.SMEM((boards,), jnp.int32),
            pltpu.VMEM((boards // chunk, chunk, board_cards.shape[1]), jnp.int32),
            pltpu.VMEM((boards // chunk, chunk, hands), jnp.int32),
            pltpu.VMEM(cards.shape, cards.dtype),
            pltpu.VMEM(left.shape, left.dtype),
            pltpu.VMEM(right.shape, right.dtype),
            dma((10,)),
            pltpu.VMEM((depths, chunk, width), f32),
            pltpu.VMEM((depths, chunk, width), f32),
            pltpu.VMEM((depths, chunk, width), f32),
            pltpu.VMEM((depths, chunk, width), f32),
            pltpu.VMEM((depths, 2, width), f32),
            pltpu.VMEM((groups, depths, 2, width), f32),
            pltpu.VMEM((2, width, width), jnp.bfloat16),
            pltpu.VMEM((chunk, width, width), jnp.bfloat16),
            pltpu.VMEM((chunk, 2 * depths, width), f32),
            pltpu.VMEM((chunk, 2 * depths, width), f32),
            pltpu.VMEM((boards, nodes, width), f32),
            pltpu.VMEM((boards, nodes, hands), f32),
            dma((depths,)),
            dma((depths,)),
            dma((depths,)),
            dma((depths,)),
            dma((depths,)),
            dma((depths,)),
            dma((groups, depths)),
            dma((groups, depths)),
        ],
        compiler_params=pltpu.CompilerParams(
            collective_id=0, has_side_effects=True, vmem_limit_bytes=42 * 1024 * 1024
        ),
    )(*(pltpu.with_memory_space_constraint(operand, pltpu.HBM) for operand in operands))
    whole = [out[None] for out in outs]
    return pl.pallas_call(
        write_out,
        out_shape=tuple(jax.ShapeDtypeStruct(out.shape, f32) for out in whole),
        in_specs=[pl.BlockSpec(memory_space=pl.ANY)] * 3,
        out_specs=tuple(pl.BlockSpec(memory_space=pl.ANY) for _ in whole),
        scratch_shapes=[dma((3,))],
        compiler_params=pltpu.CompilerParams(vmem_limit_bytes=1024 * 1024),
    )(*whole)


def solution(mesh):
    return jax.shard_map(
        functools.partial(local, mesh.shape["section"], mesh.shape["board"]),
        mesh=mesh,
        in_specs=(
            P(),
            P(),
            P("section", "board", None, None),
            P("section", "board", None, None),
            P("board"),
            P("board", None),
            P("board", None),
        ),
        out_specs=(
            P("section", "board", None, None),
            P("section", "board", None, None),
            P("section", None, None, None),
        ),
        check_vma=False,
    )
```
